32 devices in a mesh: rep: 2 (over y), tp: 4 (over z), ep: 4 (over x, core).
Axes of the slice: x: 2, y: 2, z: 4, core: 2. Of those that a mesh axis runs over, the one named last changes fastest.
Arguments:
- tokens: bfloat16 [768, 3072], P(('rep', 'ep'), 'tp'), parts along dimension 0, may hold values from -6 to 6
- routing: int32 [768, 2], P(('rep', 'ep')), parts along dimension 0, may hold values from 0 to 3, all different within a row; in each aligned block of 96 rows (0 to 95, 96 to 191, ...) at most 54 rows name the same one
- route_gates: float32 [768, 2], P(('rep', 'ep')), parts along dimension 0, may hold values from 0.2 to 1
- expert_gate: bfloat16 [4, 3072, 8192], P('ep', None, 'tp'), may hold values from -0.109375 to 0.109375
- expert_up: bfloat16 [4, 3072, 8192], P('ep', None, 'tp'), may hold values from -0.109375 to 0.109375
- expert_down: bfloat16 [4, 8192, 3072], P('ep', 'tp'), may hold values from -0.0625 to 0.0625
Outputs:
- mixture: bfloat16 [768, 3072], P(('rep', 'ep'), 'tp'), parts along dimension 0
The draws below stay inside these ranges and needn't reach their ends.
There are 2 independent parts, one for each index of `rep`. The reference program is written for one: setup_inputs(seed, part) draws one part's arguments, and reference() takes and returns one part's arrays. A program takes and returns all parts, laid end to end along the dimension named above; an argument that names none is the same for every part. Nothing has to cross between parts.
Inputs may be any that keep to these rules, and one draw needn't show every extreme that they name: `routing`: each token names two different experts. In each aligned block of 96 tokens (the rows of one index of ep) no expert is named by more than 54 tokens, a bound that some block reaches.
All inputs are finite; a program needn't handle non-finite values.
Results may differ from the reference program's by a relative error of at most 0.0085.
Values may be sent and summed in bfloat16 or wider, within the bound.
A program may use at most 128 MiB of HBM per device.

```python
import math
import jax
import jax.numpy as jnp
import numpy as np
from jax import lax

D = 3072
FF = 8192
TOK_DEV = 96
EXPERTS = 4
CAP = 54
TOKENS = 384


def shard_levels(key, extent, split, least, top_value):
    factor_of, own = 1.0, jax.random.fold_in(key, 6)
    for dim, blocks in split:
        draws = jnp.exp(jax.random.uniform(jax.random.fold_in(own, dim), (blocks,), jnp.float32, least / len(split), top_value / len(split)))
        factor_of = factor_of * jnp.repeat(draws, extent[dim] // blocks).reshape([-1 if axis == dim else 1 for axis in range(len(extent))])
    return factor_of


def routed_block(rng, own, number, rows, number_of, top, limit, slope):
    order = jax.random.permutation(rng, number_of)
    heavy_load, ordinary = load_shares(number_of, rows * top, limit, slope, True), load_shares(number_of, rows * top, limit, slope, False)
    places = jnp.arange(number_of)

    def named(sizes, offset_by):
        used = int((sizes > 0).sum())
        fixed = max(1, used // 4)
        moved = fixed + (places - fixed + offset_by * (used - fixed)) % max(1, number_of - fixed)
        return jnp.zeros((number_of,), jnp.int32).at[order[jnp.where(places < fixed, places, moved)]].set(jnp.asarray(sizes, jnp.int32))

    sizes = jnp.where(number % 4 == 0, named(heavy_load, number // 4), named(ordinary, number - number // 4 - 1))
    mixed = jax.random.permutation(jax.random.fold_in(own, 3), number_of)
    giver, sink = mixed[0:number_of // 2 * 2:2], mixed[1:number_of // 2 * 2:2]
    room = jnp.minimum(sizes[giver] - 1, limit - sizes[sink]) // 2
    room = jnp.where((giver == order[0]) | (sink == order[0]) | (sizes[sink] == 0), 0, jnp.maximum(room, 0))
    moved = jax.random.randint(jax.random.fold_in(own, 4), (number_of // 2,), 0, 1 << 20) % (room + 1)
    sizes = sizes.at[giver].add(-moved).at[sink].add(moved)
    members = jnp.searchsorted(jnp.cumsum(sizes), jnp.arange(rows * top), side="right").astype(jnp.int32)
    grid = members.reshape(top, rows).T
    grid = grid[jax.random.permutation(jax.random.fold_in(own, 1), rows)]
    offset_by = jax.random.randint(jax.random.fold_in(own, 2), (rows, 1), 0, top)
    return jnp.take_along_axis(grid, (jnp.arange(top)[None, :] + offset_by) % top, axis=1)


def load_shares(number_of, total, most, slope, full):
    portions = [(1 << 20) // math.isqrt(rank ** slope) + 1 for rank in range(1, number_of + 1)]
    largest = most if full else min(most, max(-(-total // number_of), total * portions[0] // sum(portions)))
    least = 1 if total - largest >= number_of - 1 else 0
    holding, spare = [largest] + [least] * (number_of - 1), total - largest - least * (number_of - 1)
    while spare > 0:
        movable = [i for i in range(1, number_of) if holding[i] < largest] or [i for i in range(1, number_of) if holding[i] < most]
        mass, remaining = sum([portions[i] for i in movable]), spare
        for i in movable:
            addition = min(most - holding[i], max(1, remaining * portions[i] // mass), spare)
            holding[i] = holding[i] + addition
            spare = spare - addition
    return np.array(holding)


def gaussian(stream_key, extent, scale, most, cuts=(), held_as=jnp.bfloat16):
    result = jax.random.normal(stream_key, extent, jnp.float32) * scale
    if len(cuts) > 0:
        result = shard_levels(stream_key, extent, cuts, -0.22, 0.18) * result
    return jnp.clip(result, min=-most, max=most).astype(held_as)


def setup_inputs(seed: int = 0, part: int = 0) -> dict:
    seeds = jax.random.split(jax.random.key(seed), 7)
    part_splits = jax.random.split(jax.random.fold_in(seeds[6], part), 7)
    tokens = gaussian(part_splits[0], (TOKENS, D), 1.0, 6.0, ((0, 4), (1, 4)))
    routing_keys = jax.random.split(jax.random.fold_in(part_splits[1], 1), TOKENS // TOK_DEV)
    routing_turns = jax.random.permutation(jax.random.fold_in(part_splits[1], 3), TOKENS // TOK_DEV)
    routing = jax.vmap(lambda own, number: routed_block(jax.random.fold_in(part_splits[1], 2), own, number, TOK_DEV, EXPERTS, 2, CAP, 2))(routing_keys, routing_turns).reshape((TOKENS, 2))
    route_gates = jnp.clip(0.2 + 0.8 * jax.random.uniform(part_splits[2], (TOKENS, 2), jnp.float32) ** shard_levels(part_splits[2], (TOKENS, 2), ((0, 4),), -0.2, 0.2), 0.2, 1.0)
    expert_gate = gaussian(seeds[3], (EXPERTS, D, FF), D ** -0.5, 0.109375, ((0, 4), (2, 4)))
    expert_up = gaussian(seeds[4], (EXPERTS, D, FF), D ** -0.5, 0.109375, ((0, 4), (2, 4)))
    expert_down = gaussian(seeds[5], (EXPERTS, FF, D), FF ** -0.5, 0.0625, ((0, 4), (1, 4)))
    return {"tokens": tokens, "routing": routing, "route_gates": route_gates, "expert_gate": expert_gate, "expert_up": expert_up, "expert_down": expert_down}


def slot_tables(routing, route_gates):
    count_rows = routing.shape[0]
    choices_n = routing.shape[1]
    flat_ids = routing.reshape(-1).astype(jnp.int32)
    onehot = (flat_ids[:, None] == jnp.arange(EXPERTS, dtype=jnp.int32)[None, :]).astype(jnp.int32)
    before = jnp.cumsum(onehot, axis=0) - onehot
    position = jnp.sum(before * onehot, axis=1)
    slot_index = flat_ids * CAP + position
    picked = (slot_index[:, None] == jnp.arange(EXPERTS * CAP, dtype=jnp.int32)[None, :]).astype(jnp.float32)
    dispatch = picked.reshape(count_rows, choices_n, EXPERTS * CAP).sum(axis=1)
    combine = (picked * route_gates.reshape(-1)[:, None]).reshape(count_rows, choices_n, EXPERTS * CAP).sum(axis=1)
    return dispatch, combine


def one_expert(operands):
    row_block, w_gate, w_upward, w_down = operands
    gate_part = jnp.dot(row_block, w_gate, preferred_element_type=jnp.float32)
    upward = jnp.dot(row_block, w_upward, preferred_element_type=jnp.float32)
    hidden = (jax.nn.silu(gate_part) * upward).astype(jnp.bfloat16)
    return jnp.dot(hidden, w_down, preferred_element_type=jnp.float32).astype(jnp.bfloat16)


def reference(tokens, routing, route_gates, expert_gate, expert_up, expert_down):
    blocks = TOKENS // TOK_DEV
    dispatch, combine = jax.vmap(slot_tables)(routing.reshape(blocks, TOK_DEV, 2), route_gates.reshape(blocks, TOK_DEV, 2))
    block_tokens = tokens.reshape(blocks, TOK_DEV, D).astype(jnp.float32)
    packed = jnp.einsum('btc,btd->bcd', dispatch, block_tokens, precision=lax.Precision.HIGHEST).astype(jnp.bfloat16)
    expert_rows = packed.reshape(blocks, EXPERTS, CAP, D).transpose(1, 0, 2, 3).reshape(EXPERTS, blocks * CAP, D)
    expert_out = lax.map(one_expert, (expert_rows, expert_gate, expert_up, expert_down))
    back = expert_out.reshape(EXPERTS, blocks, CAP, D).transpose(1, 0, 2, 3).reshape(blocks, EXPERTS * CAP, D)
    mixed = jnp.einsum('btc,bcd->btd', combine, back.astype(jnp.float32), precision=lax.Precision.HIGHEST)
    return mixed.reshape(TOKENS, D).astype(jnp.bfloat16)
```

```python
import functools

import jax
import jax.numpy as jnp
from jax import lax
from jax.experimental import pallas as pl
from jax.experimental.pallas import tpu as pltpu
from jax.sharding import PartitionSpec as P


def slot_tables(routing, route_gates, experts, capacity):
    count_rows = routing.shape[0]
    choices_n = routing.shape[1]
    flat_ids = routing.reshape(-1)
    onehot = (flat_ids[:, None] == jnp.arange(experts, dtype=jnp.int32)[None, :]).astype(jnp.int32)
    before = jnp.cumsum(onehot, axis=0) - onehot
    position = jnp.sum(before * onehot, axis=1)
    slot_index = flat_ids * capacity + position
    picked = (
        slot_index[:, None] == jnp.arange(experts * capacity, dtype=jnp.int32)[None, :]
    ).astype(jnp.float32)
    dispatch = picked.reshape(count_rows, choices_n, experts * capacity).sum(axis=1)
    combine = (
        (picked * route_gates.reshape(-1)[:, None])
        .reshape(count_rows, choices_n, experts * capacity)
        .sum(axis=1)
    )
    return (dispatch, combine)


def hidden_rows(everyone, expert_gate, expert_up, capacity):
    local_count = expert_gate.shape[0]
    total = everyone.shape[0]
    row_block = everyone.reshape(
        total // (local_count * capacity), local_count, capacity, everyone.shape[1]
    )
    gate_part = jnp.einsum(
        "tlcd,ldf->tlcf", row_block, expert_gate, preferred_element_type=jnp.float32
    )
    upward = jnp.einsum("tlcd,ldf->tlcf", row_block, expert_up, preferred_element_type=jnp.float32)
    return (jax.nn.silu(gate_part) * upward).astype(jnp.bfloat16)


def plain_body(tokens, routing, route_gates, expert_gate, expert_up, expert_down):
    local_count = expert_gate.shape[0]
    ep_count = lax.axis_size("ep")
    tp_count = lax.axis_size("tp")
    tok_count = tokens.shape[0]
    capacity = 2 * tok_count // ep_count + tok_count // 16
    experts = local_count * ep_count
    dispatch, combine = slot_tables(routing, route_gates, experts, capacity)
    dispatch_low = dispatch.astype(jnp.bfloat16)
    whole = lax.all_gather(tokens, "tp", axis=1, tiled=True)
    packed = jnp.einsum(
        "tc,td->cd", dispatch_low, whole, preferred_element_type=jnp.float32
    ).astype(jnp.bfloat16)
    everyone = lax.all_to_all(packed, "ep", split_axis=0, concat_axis=0, tiled=True)
    total_rows = everyone.shape[0]
    columns = everyone.shape[1]
    hidden = hidden_rows(everyone, expert_gate, expert_up, capacity)
    part = jnp.einsum("tlcf,lfd->dtlc", hidden, expert_down, preferred_element_type=jnp.float32)
    summed_t = lax.psum_scatter(
        part.reshape(columns // tp_count * lax.axis_size("tp"), total_rows),
        "tp",
        scatter_dimension=0,
        tiled=True,
    )
    summed = summed_t.T
    expert_out = summed.astype(jnp.bfloat16)
    returned = lax.all_to_all(expert_out, "ep", split_axis=0, concat_axis=0, tiled=True)
    mixed = jnp.dot(combine, returned.astype(jnp.float32), precision=lax.Precision.HIGHEST)
    return mixed.astype(jnp.bfloat16)


MESH = pl.DeviceIdType.MESH
LANES = 128


def up_to(value, step):
    return -(-value // step) * step


def rcopy(src, dst, send, recv, device):
    return pltpu.make_async_remote_copy(
        src_ref=src, dst_ref=dst, send_sem=send, recv_sem=recv, device_id=device, device_id_type=MESH
    )


def layer_kernel(
    tp, ep, cap, rows, tokens, meta, gate_hbm, up_hbm, down_hbm, out,
    x, m, pick, place, scale, wg, wu, wd, acc_g, acc_u, packed, hidden, part,
    c, c_in, x_out, x_in, z_out, z_in,
    w_sem, zs, zr, xs, xr, cs, cr, ms, mr, rcs, rcr, rxs, rxr, rzs, rzr,
):
    t = lax.axis_index("tp")
    e = lax.axis_index("ep")
    half = ep // 2
    core = lax.rem(e, 2)
    column = e // 2
    e_core = e + 1 - 2 * core
    e_x = lax.rem(e + half, ep)
    e_xc = lax.rem(e_core + half, ep)
    tok, feat = tokens.shape
    ff = wg.shape[2]
    f32, b16 = jnp.float32, jnp.bfloat16

    def quarter(d):
        return lax.rem(t + tp - d, tp)

    loads = []
    for d in range(tp):
        q = quarter(d)
        for k, (src, dst) in enumerate(((gate_hbm, wg), (up_hbm, wu))):
            r = pl.ds(pl.multiple_of(q * feat, feat), feat)
            loads.append(pltpu.make_async_copy(src.at[0, r, :], dst.at[q], w_sem.at[k * tp + d]))
    down_loads = []
    for i in range(tp):
        q = quarter(tp - 1 - i)
        r = pl.ds(pl.multiple_of(q * feat, feat), feat)
        down_loads.append(pltpu.make_async_copy(down_hbm.at[0, :, r], wd.at[q], w_sem.at[2 * tp + i]))
    for load in loads + down_loads:
        load.start()

    pad = x.shape[2] - tok
    for q in range(tp):
        for b in range(ep):
            x[q, b, tok:, :] = jnp.zeros((pad, feat), b16)
    x[t, e, 0:tok, :] = tokens[...]
    m[e] = meta[...]
    part[rows:, :] = jnp.zeros((part.shape[0] - rows, feat), b16)

    barrier = pltpu.get_barrier_semaphore()
    for d in range(1, tp):
        pl.semaphore_signal(barrier, inc=1, device_id={"tp": lax.rem(t + d, tp)}, device_id_type=MESH)
    pl.semaphore_signal(barrier, inc=1, device_id={"ep": e_x}, device_id_type=MESH)
    pl.semaphore_signal(barrier, inc=1, device_id={"ep": e_core}, device_id_type=MESH)
    pl.semaphore_wait(barrier, tp + 1)

    sent = []

    def send(src, dst, s, r, device):
        copy = rcopy(src, dst, s, r, device)
        copy.start()
        sent.append(copy)

    def block(q, b):
        return x.at[q, b, pl.ds(0, tok), :]

    to_x, to_core = {"ep": e_x}, {"ep": e_core}
    send(meta, m.at[e], ms.at[0], mr.at[0], to_x)
    send(meta, m.at[e], ms.at[1], mr.at[1], to_core)
    send(tokens, block(t, e), xs.at[0], xr.at[0], to_x)
    for d in range(1, tp):
        send(tokens, block(t, e), zs.at[d], zr.at[d], {"tp": lax.rem(t + d, tp)})
    send(tokens, block(t, e), cs.at[0], cr.at[0], to_core)

    def got(dst, s, r, device):
        rcopy(dst, dst, s, r, device).wait_recv()

    def take_z(d):
        q = quarter(d)
        got(block(q, e), zs.at[d], zr.at[d], {"tp": q})
        send(block(q, e), block(q, e), xs.at[d], xr.at[d], to_x)
        send(block(q, e), block(q, e), cs.at[d], cr.at[d], to_core)

    def take_x(d):
        q = quarter(d)
        got(block(q, e_x), xs.at[d], xr.at[d], to_x)
        send(block(q, e_x), block(q, e_x), cs.at[tp + d], cr.at[tp + d], to_core)

    def take_core(d):
        q = quarter(d)
        got(block(q, e_core), cs.at[d], cr.at[d], to_core)
        got(block(q, e_xc), cs.at[tp + d], cr.at[tp + d], to_core)

    got(m.at[e_x], ms.at[0], mr.at[0], to_x)
    send(m.at[e_x], m.at[e_x], ms.at[2], mr.at[2], to_core)
    got(m.at[e_core], ms.at[1], mr.at[1], to_core)
    got(m.at[e_xc], ms.at[2], mr.at[2], to_core)

    slots = pick.shape[0]
    mine = e.astype(f32)
    earlier = (
        lax.broadcasted_iota(jnp.int32, (LANES, LANES), 0)
        < lax.broadcasted_iota(jnp.int32, (LANES, LANES), 1)
    ).astype(b16)
    slot = lax.broadcasted_iota(jnp.int32, (slots, LANES), 0).astype(f32)
    total = jnp.zeros((slots, 1), f32)
    for b in range(ep):
        first, second = m[b, 0:1, :] == mine, m[b, 1:2, :] == mine
        named = jnp.where(first, 1.0, 0.0) + jnp.where(second, 1.0, 0.0)
        weight = jnp.where(first, m[b, 2:3, :], 0.0) + jnp.where(second, m[b, 3:4, :], 0.0)
        spread = jnp.broadcast_to(named, (16, LANES)).astype(b16)
        position = jnp.dot(spread, earlier, preferred_element_type=f32)[0:1, :]
        where_to = jnp.where(named > 0.5, position + float(b * cap), -1.0)
        chosen = jnp.where(slot == where_to, 1.0, 0.0)
        total = total + jnp.sum(chosen * weight, axis=1, keepdims=True)
        pick[:, b * LANES:(b + 1) * LANES] = chosen.astype(b16)
        at = ((b % 2) * half + b // 2) * tok
        place[at:at + tok, :] = chosen.T[0:tok, :].astype(b16)
    scale[...] = jnp.broadcast_to(total, scale.shape)

    step = 512
    tiles = ff // step

    def project(d, last):
        q = quarter(d)
        loads[2 * d].wait()
        loads[2 * d + 1].wait()
        everyone = x[q].reshape(ep * x.shape[2], feat)
        packed[...] = jnp.dot(pick[0:rows, :], everyone, preferred_element_type=f32).astype(b16)

        def tile(j, carry):
            cols = pl.ds(pl.multiple_of(j * step, step), step)
            g = jnp.dot(packed[...], wg[q, :, cols], preferred_element_type=f32)
            u = jnp.dot(packed[...], wu[q, :, cols], preferred_element_type=f32)
            if d > 0:
                g = g + acc_g[:, cols]
                u = u + acc_u[:, cols]
            if last:
                h = g / (1.0 + jnp.exp(-g)) * u * scale[0:rows, 0:1]
                hidden[:, cols] = h.astype(b16)
            else:
                acc_g[:, cols] = g
                acc_u[:, cols] = u
            return carry

        lax.fori_loop(0, tiles, tile, 0)

    take_x(0)
    for d in range(1, tp):
        take_z(d)
        if d > 1:
            take_x(d - 1)
        take_core(d - 1)
        project(d - 1, False)
    take_x(tp - 1)
    take_core(tp - 1)
    project(tp - 1, True)

    width = 256 if feat % 256 == 0 else LANES

    def to_tokens(i):
        q = quarter(tp - 1 - i)
        down_loads[i].wait()

        def tile(j, carry):
            cols = pl.ds(pl.multiple_of(j * width, width), width)
            part[0:rows, cols] = jnp.dot(hidden[...], wd[q, :, cols], preferred_element_type=f32).astype(b16)
            back = jnp.dot(place[...], part[:, cols], preferred_element_type=f32).astype(b16)
            c[i, :, :, cols] = back.reshape(ep, tok, width)
            return carry

        lax.fori_loop(0, feat // width, tile, 0)
        away = pl.ds((1 - core) * half, half)
        send(c.at[i, away], c_in.at[i], rcs.at[i], rcr.at[i], to_core)

    def sum_core(i):
        got(c_in.at[i], rcs.at[i], rcr.at[i], to_core)
        far = 1 - column
        value = c[i, core * half + far].astype(f32) + c_in[i, far].astype(f32)
        x_out[i] = value.astype(b16)
        send(x_out.at[i], x_in.at[i], rxs.at[i], rxr.at[i], to_x)

    def sum_x(i):
        got(x_in.at[i], rxs.at[i], rxr.at[i], to_x)
        value = c[i, core * half + column].astype(f32) + c_in[i, column].astype(f32)
        return value + x_in[i].astype(f32)

    for i in range(tp):
        to_tokens(i)
        if i > 0:
            sum_core(i - 1)
    sum_core(tp - 1)
    for i in range(tp - 1):
        z_out[i] = sum_x(i).astype(b16)
        send(z_out.at[i], z_in.at[i], rzs.at[i], rzr.at[i], {"tp": quarter(tp - 1 - i)})
    result = sum_x(tp - 1)
    for i in range(tp - 1):
        got(z_in.at[i], rzs.at[i], rzr.at[i], {"tp": lax.rem(t + tp - 1 - i, tp)})
        result = result + z_in[i].astype(f32)
    out[...] = result.astype(b16)
    for copy in sent:
        copy.wait_send()


def kernel_body(tokens, routing, route_gates, expert_gate, expert_up, expert_down):
    ep, tp = lax.axis_size("ep"), lax.axis_size("tp")
    tok, feat = tokens.shape
    ff = expert_gate.shape[2]
    cap = 2 * tok // ep + tok // 16
    rows = up_to(ep * cap, 16)
    slots = up_to(rows, LANES)
    ids = jnp.pad(routing.astype(jnp.float32).T, ((0, 0), (0, LANES - tok)), constant_values=-1.0)
    weights = jnp.pad(route_gates.T, ((0, 4), (0, LANES - tok)))
    meta = jnp.concatenate([ids, weights], axis=0)
    f32, b16 = jnp.float32, jnp.bfloat16
    dma = pltpu.SemaphoreType.DMA
    vmem = pl.BlockSpec(memory_space=pltpu.VMEM)
    hbm = pl.BlockSpec(memory_space=pl.ANY)
    return pl.pallas_call(
        functools.partial(layer_kernel, tp, ep, cap, rows),
        out_shape=jax.ShapeDtypeStruct((tok, feat), b16),
        in_specs=[vmem, vmem, hbm, hbm, hbm],
        out_specs=vmem,
        scratch_shapes=[
            pltpu.VMEM((tp, ep, LANES, feat), b16),
            pltpu.VMEM((ep, 8, LANES), f32),
            pltpu.VMEM((slots, ep * LANES), b16),
            pltpu.VMEM((ep * tok, slots), b16),
            pltpu.VMEM((slots, LANES), f32),
            pltpu.VMEM((tp, feat, ff), b16),
            pltpu.VMEM((tp, feat, ff), b16),
            pltpu.VMEM((tp, ff, feat), b16),
            pltpu.VMEM((rows, ff), f32),
            pltpu.VMEM((rows, ff), f32),
            pltpu.VMEM((rows, feat), b16),
            pltpu.VMEM((rows, ff), b16),
            pltpu.VMEM((slots, feat), b16),
            pltpu.VMEM((tp, ep, tok, feat), b16),
            pltpu.VMEM((tp, ep // 2, tok, feat), b16),
            pltpu.VMEM((tp, tok, feat), b16),
            pltpu.VMEM((tp, tok, feat), b16),
            pltpu.VMEM((tp, tok, feat), b16),
            pltpu.VMEM((tp, tok, feat), b16),
            dma((3 * tp,)),
            dma((tp,)), dma((tp,)),
            dma((tp,)), dma((tp,)),
            dma((2 * tp,)), dma((2 * tp,)),
            dma((3,)), dma((3,)),
            dma((tp,)), dma((tp,)),
            dma((tp,)), dma((tp,)),
            dma((tp,)), dma((tp,)),
        ],
        compiler_params=pltpu.CompilerParams(
            collective_id=0, has_side_effects=True, vmem_limit_bytes=60 * 1024 * 1024
        ),
    )(tokens, meta, expert_gate, expert_up, expert_down)


def body(tokens, routing, route_gates, expert_gate, expert_up, expert_down):
    ep, tp = lax.axis_size("ep"), lax.axis_size("tp")
    tok, feat = tokens.shape
    ff = expert_gate.shape[2]
    fits = ep == 4 and expert_gate.shape[0] == 1 and tok <= LANES and tok % 16 == 0
    fits = fits and feat % LANES == 0 and ff % 512 == 0 and 3 * tp * feat * ff * 2 <= 40 << 20
    run = kernel_body if fits else plain_body
    return run(tokens, routing, route_gates, expert_gate, expert_up, expert_down)


def solution(mesh):
    return jax.shard_map(
        body,
        mesh=mesh,
        in_specs=(
            P(("rep", "ep"), "tp"),
            P(("rep", "ep"), None),
            P(("rep", "ep"), None),
            P("ep", None, "tp"),
            P("ep", None, "tp"),
            P("ep", "tp", None),
        ),
        out_specs=P(("rep", "ep"), "tp"),
        check_vma=False,
    )
```

```python
import functools

import jax
import jax.numpy as jnp
from jax import lax
from jax.experimental import pallas as pl
from jax.experimental.pallas import tpu as pltpu
from jax.sharding import PartitionSpec as P


def slot_tables(routing, route_gates, experts, capacity):
    count_rows = routing.shape[0]
    choices_n = routing.shape[1]
    flat_ids = routing.reshape(-1)
    onehot = (flat_ids[:, None] == jnp.arange(experts, dtype=jnp.int32)[None, :]).astype(jnp.int32)
    before = jnp.cumsum(onehot, axis=0) - onehot
    position = jnp.sum(before * onehot, axis=1)
    slot_index = flat_ids * capacity + position
    picked = (
        slot_index[:, None] == jnp.arange(experts * capacity, dtype=jnp.int32)[None, :]
    ).astype(jnp.float32)
    dispatch = picked.reshape(count_rows, choices_n, experts * capacity).sum(axis=1)
    combine = (
        (picked * route_gates.reshape(-1)[:, None])
        .reshape(count_rows, choices_n, experts * capacity)
        .sum(axis=1)
    )
    return (dispatch, combine)


def hidden_rows(everyone, expert_gate, expert_up, capacity):
    local_count = expert_gate.shape[0]
    total = everyone.shape[0]
    row_block = everyone.reshape(
        total // (local_count * capacity), local_count, capacity, everyone.shape[1]
    )
    gate_part = jnp.einsum(
        "tlcd,ldf->tlcf", row_block, expert_gate, preferred_element_type=jnp.float32
    )
    upward = jnp.einsum("tlcd,ldf->tlcf", row_block, expert_up, preferred_element_type=jnp.float32)
    return (jax.nn.silu(gate_part) * upward).astype(jnp.bfloat16)


def plain_body(tokens, routing, route_gates, expert_gate, expert_up, expert_down):
    local_count = expert_gate.shape[0]
    ep_count = lax.axis_size("ep")
    tp_count = lax.axis_size("tp")
    tok_count = tokens.shape[0]
    capacity = 2 * tok_count // ep_count + tok_count // 16
    experts = local_count * ep_count
    dispatch, combine = slot_tables(routing, route_gates, experts, capacity)
    dispatch_low = dispatch.astype(jnp.bfloat16)
    whole = lax.all_gather(tokens, "tp", axis=1, tiled=True)
    packed = jnp.einsum(
        "tc,td->cd", dispatch_low, whole, preferred_element_type=jnp.float32
    ).astype(jnp.bfloat16)
    everyone = lax.all_to_all(packed, "ep", split_axis=0, concat_axis=0, tiled=True)
    total_rows = everyone.shape[0]
    columns = everyone.shape[1]
    hidden = hidden_rows(everyone, expert_gate, expert_up, capacity)
    part = jnp.einsum("tlcf,lfd->dtlc", hidden, expert_down, preferred_element_type=jnp.float32)
    summed_t = lax.psum_scatter(
        part.reshape(columns // tp_count * lax.axis_size("tp"), total_rows),
        "tp",
        scatter_dimension=0,
        tiled=True,
    )
    summed = summed_t.T
    expert_out = summed.astype(jnp.bfloat16)
    returned = lax.all_to_all(expert_out, "ep", split_axis=0, concat_axis=0, tiled=True)
    mixed = jnp.dot(combine, returned.astype(jnp.float32), precision=lax.Precision.HIGHEST)
    return mixed.astype(jnp.bfloat16)


MESH = pl.DeviceIdType.MESH
LANES = 128


def up_to(value, step):
    return -(-value // step) * step


def rcopy(src, dst, send, recv, device):
    return pltpu.make_async_remote_copy(
        src_ref=src, dst_ref=dst, send_sem=send, recv_sem=recv, device_id=device, device_id_type=MESH
    )


def layer_kernel(
    tp, ep, cap, rows, tokens, meta, gate_hbm, up_hbm, down_hbm, out,
    x, m, pick, place, scale, wg, wu, wd, acc_g, acc_u, packed, hidden, part,
    c, c_in, x_out, x_in, z_out, z_in,
    w_sem, zs, zr, xs, xr, cs, cr, ms, mr, rcs, rcr, rxs, rxr, rzs, rzr,
):
    t = lax.axis_index("tp")
    e = lax.axis_index("ep")
    half = ep // 2
    core = lax.rem(e, 2)
    column = e // 2
    e_core = e + 1 - 2 * core
    e_x = lax.rem(e + half, ep)
    e_xc = lax.rem(e_core + half, ep)
    tok, feat = tokens.shape
    ff = wg.shape[2]
    f32, b16 = jnp.float32, jnp.bfloat16

    def quarter(d):
        return lax.rem(t + tp - d, tp)

    def select(values):
        found = jnp.int32(values[0])
        for k in range(1, tp):
            found = jnp.where(t == k, jnp.int32(values[k]), found)
        return found

    nearest = [sorted(range(tp), key=lambda q, k=k: (abs(q - k), q)) for k in range(tp)]
    arrivals = [select([nearest[k][i] for k in range(tp)]) for i in range(tp)]
    pieces = 2 if tok % 32 == 0 else 1
    piece = tok // pieces

    loads = []
    for d in range(tp):
        q = arrivals[d]
        for k, (src, dst) in enumerate(((gate_hbm, wg), (up_hbm, wu))):
            r = pl.ds(pl.multiple_of(q * feat, feat), feat)
            loads.append(pltpu.make_async_copy(src.at[0, r, :], dst.at[q], w_sem.at[k * tp + d]))
    down_loads = []
    for i in range(tp):
        q = quarter(tp - 1 - i)
        r = pl.ds(pl.multiple_of(q * feat, feat), feat)
        down_loads.append(pltpu.make_async_copy(down_hbm.at[0, :, r], wd.at[q], w_sem.at[2 * tp + i]))
    for load in loads + down_loads:
        load.start()

    pad = x.shape[2] - tok
    for q in range(tp):
        for b in range(ep):
            x[q, b, tok:, :] = jnp.zeros((pad, feat), b16)
    x[t, e, 0:tok, :] = tokens[...]
    m[e] = meta[...]
    part[rows:, :] = jnp.zeros((part.shape[0] - rows, feat), b16)

    barrier = pltpu.get_barrier_semaphore()
    for d in range(1, tp):
        pl.semaphore_signal(barrier, inc=1, device_id={"tp": lax.rem(t + d, tp)}, device_id_type=MESH)
    pl.semaphore_signal(barrier, inc=1, device_id={"ep": e_x}, device_id_type=MESH)
    pl.semaphore_signal(barrier, inc=1, device_id={"ep": e_core}, device_id_type=MESH)
    pl.semaphore_wait(barrier, tp + 1)

    sent = []

    def send(src, dst, s, r, device):
        copy = rcopy(src, dst, s, r, device)
        copy.start()
        sent.append(copy)

    def block(q, b, p):
        return x.at[q, b, pl.ds(p * piece, piece), :]

    some = []

    def send_if(cond, src, dst, s, r, device):
        copy = rcopy(src, dst, s, r, device)
        some.append((cond, copy))

        @pl.when(cond)
        def _():
            copy.start()

    to_x, to_core = {"ep": e_x}, {"ep": e_core}
    send(meta, m.at[e], ms.at[0], mr.at[0], to_x)
    send(meta, m.at[e], ms.at[1], mr.at[1], to_core)
    above, below = {"tp": lax.rem(t + 1, tp)}, {"tp": lax.rem(t + tp - 1, tp)}
    for p in range(pieces):
        own = tokens.at[pl.ds(p * piece, piece), :]
        n = pieces * t + p
        send_if(t < tp - 1, own, block(t, e, p), zs.at[n], zr.at[n], above)
        send_if(t > 0, own, block(t, e, p), zs.at[pieces * tp + n], zr.at[n], below)
        send(own, block(t, e, p), xs.at[n], xr.at[n], to_x)
        send(own, block(t, e, p), cs.at[n], cr.at[n], to_core)

    def got(dst, s, r, device):
        rcopy(dst, dst, s, r, device).wait_recv()

    def take_z(i):
        q = arrivals[i]
        for p in range(pieces):
            n = pieces * q + p
            one = block(q, e, p)
            got(one, zs.at[n], zr.at[n], above)
            send_if((q < t) & (t < tp - 1), one, one, zs.at[n], zr.at[n], above)
            send_if((q > t) & (t > 0), one, one, zs.at[pieces * tp + n], zr.at[n], below)
            send(one, one, xs.at[n], xr.at[n], to_x)
            send(one, one, cs.at[n], cr.at[n], to_core)

    def take_x(i):
        for p in range(pieces):
            n = pieces * arrivals[i] + p
            far = pieces * tp + n
            one = block(arrivals[i], e_x, p)
            got(one, xs.at[n], xr.at[n], to_x)
            send(one, one, cs.at[far], cr.at[far], to_core)

    def take_core(i):
        for p in range(pieces):
            n = pieces * arrivals[i] + p
            far = pieces * tp + n
            got(block(arrivals[i], e_core, p), cs.at[n], cr.at[n], to_core)
            got(block(arrivals[i], e_xc, p), cs.at[far], cr.at[far], to_core)

    got(m.at[e_x], ms.at[0], mr.at[0], to_x)
    send(m.at[e_x], m.at[e_x], ms.at[2], mr.at[2], to_core)
    got(m.at[e_core], ms.at[1], mr.at[1], to_core)
    got(m.at[e_xc], ms.at[2], mr.at[2], to_core)

    slots = pick.shape[0]
    mine = e.astype(f32)
    earlier = (
        lax.broadcasted_iota(jnp.int32, (LANES, LANES), 0)
        < lax.broadcasted_iota(jnp.int32, (LANES, LANES), 1)
    ).astype(b16)
    slot = lax.broadcasted_iota(jnp.int32, (slots, LANES), 0).astype(f32)
    total = jnp.zeros((slots, 1), f32)
    for b in range(ep):
        first, second = m[b, 0:1, :] == mine, m[b, 1:2, :] == mine
        named = jnp.where(first, 1.0, 0.0) + jnp.where(second, 1.0, 0.0)
        weight = jnp.where(first, m[b, 2:3, :], 0.0) + jnp.where(second, m[b, 3:4, :], 0.0)
        spread = jnp.broadcast_to(named, (16, LANES)).astype(b16)
        position = jnp.dot(spread, earlier, preferred_element_type=f32)[0:1, :]
        where_to = jnp.where(named > 0.5, position + float(b * cap), -1.0)
        chosen = jnp.where(slot == where_to, 1.0, 0.0)
        total = total + jnp.sum(chosen * weight, axis=1, keepdims=True)
        pick[:, b * LANES:(b + 1) * LANES] = chosen.astype(b16)
        at = ((b % 2) * half + b // 2) * tok
        place[at:at + tok, :] = chosen.T[0:tok, :].astype(b16)
    scale[...] = jnp.broadcast_to(total, scale.shape)

    step = 512
    tiles = ff // step

    def project(d, last):
        q = arrivals[d]
        loads[2 * d].wait()
        loads[2 * d + 1].wait()
        everyone = x[q].reshape(ep * x.shape[2], feat)
        packed[...] = jnp.dot(pick[0:rows, :], everyone, preferred_element_type=f32).astype(b16)

        def tile(j, carry):
            cols = pl.ds(pl.multiple_of(j * step, step), step)
            g = jnp.dot(packed[...], wg[q, :, cols], preferred_element_type=f32)
            u = jnp.dot(packed[...], wu[q, :, cols], preferred_element_type=f32)
            if d > 0:
                g = g + acc_g[:, cols]
                u = u + acc_u[:, cols]
            if last:
                h = g / (1.0 + jnp.exp(-g)) * u * scale[0:rows, 0:1]
                hidden[:, cols] = h.astype(b16)
            else:
                acc_g[:, cols] = g
                acc_u[:, cols] = u
            return carry

        lax.fori_loop(0, tiles, tile, 0)

    take_x(0)
    for i in range(1, tp - 1):
        take_z(i)
    if tp > 2:
        take_x(1)
    take_core(0)
    project(0, tp == 1)
    take_z(tp - 1)
    for i in range(1, tp):
        if i + 1 < tp:
            take_x(i + 1)
        take_core(i)
        project(i, i == tp - 1)

    width = 256 if feat % 256 == 0 else LANES

    def to_tokens(i):
        q = quarter(tp - 1 - i)
        down_loads[i].wait()

        def tile(j, carry):
            cols = pl.ds(pl.multiple_of(j * width, width), width)
            part[0:rows, cols] = jnp.dot(hidden[...], wd[q, :, cols], preferred_element_type=f32).astype(b16)
            back = jnp.dot(place[...], part[:, cols], preferred_element_type=f32).astype(b16)
            c[i, :, :, cols] = back.reshape(ep, tok, width)
            return carry

        lax.fori_loop(0, feat // width, tile, 0)
        away = pl.ds((1 - core) * half, half)
        send(c.at[i, away], c_in.at[i], rcs.at[i], rcr.at[i], to_core)

    def part_of(p):
        return slice(p * piece, (p + 1) * piece)

    def sum_core(i):
        got(c_in.at[i], rcs.at[i], rcr.at[i], to_core)
        far = 1 - column
        for p in range(pieces):
            r = part_of(p)
            value = c[i, core * half + far, r].astype(f32) + c_in[i, far, r].astype(f32)
            x_out[i, r] = value.astype(b16)
            n = pieces * i + p
            view = pl.ds(p * piece, piece)
            send(x_out.at[i, view], x_in.at[i, view], rxs.at[n], rxr.at[n], to_x)

    def sum_x(i, p):
        r, n = part_of(p), pieces * i + p
        got(x_in.at[i, pl.ds(p * piece, piece)], rxs.at[n], rxr.at[n], to_x)
        value = c[i, core * half + column, r].astype(f32) + c_in[i, column, r].astype(f32)
        return value + x_in[i, r].astype(f32)

    for i in range(tp):
        to_tokens(i)
        if i > 0:
            sum_core(i - 1)
    sum_core(tp - 1)
    for i in range(tp - 1):
        for p in range(pieces):
            z_out[i, part_of(p)] = sum_x(i, p).astype(b16)
            n = pieces * i + p
            view = pl.ds(p * piece, piece)
            peer = {"tp": quarter(tp - 1 - i)}
            send(z_out.at[i, view], z_in.at[i, view], rzs.at[n], rzr.at[n], peer)
    for p in range(pieces):
        result = sum_x(tp - 1, p)
        for i in range(tp - 1):
            n = pieces * i + p
            peer = {"tp": lax.rem(t + tp - 1 - i, tp)}
            got(z_in.at[i, pl.ds(p * piece, piece)], rzs.at[n], rzr.at[n], peer)
            result = result + z_in[i, part_of(p)].astype(f32)
        out[part_of(p), :] = result.astype(b16)
    for cond, copy in some:

        @pl.when(cond)
        def _(copy=copy):
            copy.wait_send()

    for copy in sent:
        copy.wait_send()


def kernel_body(tokens, routing, route_gates, expert_gate, expert_up, expert_down):
    ep, tp = lax.axis_size("ep"), lax.axis_size("tp")
    tok, feat = tokens.shape
    ff = expert_gate.shape[2]
    cap = 2 * tok // ep + tok // 16
    rows = up_to(ep * cap, 16)
    slots = up_to(rows, LANES)
    ids = jnp.pad(routing.astype(jnp.float32).T, ((0, 0), (0, LANES - tok)), constant_values=-1.0)
    weights = jnp.pad(route_gates.T, ((0, 4), (0, LANES - tok)))
    meta = jnp.concatenate([ids, weights], axis=0)
    f32, b16 = jnp.float32, jnp.bfloat16
    dma = pltpu.SemaphoreType.DMA
    vmem = pl.BlockSpec(memory_space=pltpu.VMEM)
    hbm = pl.BlockSpec(memory_space=pl.ANY)
    return pl.pallas_call(
        functools.partial(layer_kernel, tp, ep, cap, rows),
        out_shape=jax.ShapeDtypeStruct((tok, feat), b16),
        in_specs=[vmem, vmem, hbm, hbm, hbm],
        out_specs=vmem,
        scratch_shapes=[
            pltpu.VMEM((tp, ep, LANES, feat), b16),
            pltpu.VMEM((ep, 8, LANES), f32),
            pltpu.VMEM((slots, ep * LANES), b16),
            pltpu.VMEM((ep * tok, slots), b16),
            pltpu.VMEM((slots, LANES), f32),
            pltpu.VMEM((tp, feat, ff), b16),
            pltpu.VMEM((tp, feat, ff), b16),
            pltpu.VMEM((tp, ff, feat), b16),
            pltpu.VMEM((rows, ff), f32),
            pltpu.VMEM((rows, ff), f32),
            pltpu.VMEM((rows, feat), b16),
            pltpu.VMEM((rows, ff), b16),
            pltpu.VMEM((slots, feat), b16),
            pltpu.VMEM((tp, ep, tok, feat), b16),
            pltpu.VMEM((tp, ep // 2, tok, feat), b16),
            pltpu.VMEM((tp, tok, feat), b16),
            pltpu.VMEM((tp, tok, feat), b16),
            pltpu.VMEM((tp, tok, feat), b16),
            pltpu.VMEM((tp, tok, feat), b16),
            dma((3 * tp,)),
            dma((4 * tp,)), dma((2 * tp,)),
            dma((2 * tp,)), dma((2 * tp,)),
            dma((4 * tp,)), dma((4 * tp,)),
            dma((3,)), dma((3,)),
            dma((tp,)), dma((tp,)),
            dma((2 * tp,)), dma((2 * tp,)),
            dma((2 * tp,)), dma((2 * tp,)),
        ],
        compiler_params=pltpu.CompilerParams(
            collective_id=0, has_side_effects=True, vmem_limit_bytes=60 * 1024 * 1024
        ),
    )(tokens, meta, expert_gate, expert_up, expert_down)


def body(tokens, routing, route_gates, expert_gate, expert_up, expert_down):
    ep, tp = lax.axis_size("ep"), lax.axis_size("tp")
    tok, feat = tokens.shape
    ff = expert_gate.shape[2]
    fits = ep == 4 and tp > 2 and expert_gate.shape[0] == 1 and tok <= LANES and tok % 16 == 0
    fits = fits and feat % LANES == 0 and ff % 512 == 0 and 3 * tp * feat * ff * 2 <= 40 << 20
    run = kernel_body if fits else plain_body
    return run(tokens, routing, route_gates, expert_gate, expert_up, expert_down)


def solution(mesh):
    return jax.shard_map(
        body,
        mesh=mesh,
        in_specs=(
            P(("rep", "ep"), "tp"),
            P(("rep", "ep"), None),
            P(("rep", "ep"), None),
            P("ep", None, "tp"),
            P("ep", None, "tp"),
            P("ep", "tp", None),
        ),
        out_specs=P(("rep", "ep"), "tp"),
        check_vma=False,
    )
```
